64 devices in a mesh: dp: 4 (over x, y), sp: 16 (over z, core).
Axes of the slice: x: 2, y: 2, z: 8, core: 2. Of those that a mesh axis runs over, the one named last changes fastest.
The devices are a block of a 4x4x8 slice.
Arguments:
- pixels: bfloat16 [128, 384, 512, 3], P('dp', 'sp'), parts along dimension 0
- w_stem: bfloat16 [7, 7, 3, 64], replicated
- bn_stem: float32 [2, 64], replicated
- w_a: bfloat16 [6, 3, 3, 64, 64], replicated
- bn_a: float32 [6, 2, 64], replicated
- w_down: bfloat16 [3, 3, 64, 128], replicated
- bn_down: float32 [2, 128], replicated
- w_b: bfloat16 [2, 3, 3, 128, 128], replicated
- bn_b: float32 [2, 2, 128], replicated
Outputs:
- output: bfloat16 [128, 48, 64, 128], P('dp', 'sp'), parts along dimension 0
There are 4 independent parts. The reference program is written for one: setup_inputs(seed, part) draws one part's arguments, and reference() takes and returns one part's arrays. A program takes and returns all parts, laid end to end along the dimension named above; an argument that names none is the same for every part.
All inputs are finite; a program needn't handle non-finite values.
Results may differ from the reference program's by a relative error of at most 0.019651.
Values are sent between devices in bfloat16 or wider.
A program may use at most 768 MiB of HBM per device.

```python
import jax
import jax.numpy as jnp
from jax import lax

IMAGES = 32
IMG_HEIGHT = 384
IMG_WIDTH = 512
IN_CHANS = 3
CH_A = 64
CH_B = 128
LAYERS_A = 6
LAYERS_B = 2
BN_EPS = 1e-5
CONV_DIMS = ("NHWC", "HWIO", "NHWC")


def draw_weights(key, shape):
    fan_in = shape[-4] * shape[-3] * shape[-2]
    return (jax.random.normal(key, shape, jnp.float32) * fan_in ** -0.5).astype(jnp.bfloat16)


def draw_norm(key, layers, channels):
    gain_key, shift_key = jax.random.split(key)
    gains = 1.0 + 0.25 * jax.random.normal(gain_key, (layers, 1, channels), jnp.float32)
    shifts = 0.3 * jax.random.normal(shift_key, (layers, 1, channels), jnp.float32)
    return jnp.concatenate([gains, shifts], axis=1)


def setup_inputs(seed: int = 0, part: int = 0) -> dict:
    keys = jax.random.split(jax.random.key(seed), 9)
    pix_keys = jax.random.split(jax.random.fold_in(keys[0], part), 2)
    noise = jax.random.normal(pix_keys[0], (IMAGES, IMG_HEIGHT, IMG_WIDTH, IN_CHANS), jnp.float32)
    ramp = jnp.linspace(-1.0, 1.0, IMG_HEIGHT, dtype=jnp.float32)[None, :, None, None]
    band_gain = 1.5 * jax.random.normal(pix_keys[1], (IMAGES, 1, 1, IN_CHANS), jnp.float32)
    return {
        "pixels": (noise + band_gain * ramp).astype(jnp.bfloat16),
        "w_stem": draw_weights(keys[1], (7, 7, IN_CHANS, CH_A)),
        "bn_stem": draw_norm(keys[2], 1, CH_A)[0],
        "w_a": draw_weights(keys[3], (LAYERS_A, 3, 3, CH_A, CH_A)),
        "bn_a": draw_norm(keys[4], LAYERS_A, CH_A),
        "w_down": draw_weights(keys[5], (3, 3, CH_A, CH_B)),
        "bn_down": draw_norm(keys[6], 1, CH_B)[0],
        "w_b": draw_weights(keys[7], (LAYERS_B, 3, 3, CH_B, CH_B)),
        "bn_b": draw_norm(keys[8], LAYERS_B, CH_B),
    }


def conv_full(hidden, kernel, stride):
    border = kernel.shape[0] // 2
    return lax.conv_general_dilated(hidden.astype(jnp.float32), kernel.astype(jnp.float32), (stride, stride), ((border, border), (border, border)), dimension_numbers=CONV_DIMS)


def norm_relu(conv_out, bn_pair):
    ch_mean = jnp.mean(conv_out, axis=(0, 1, 2))
    ch_var = jnp.mean(conv_out * conv_out, axis=(0, 1, 2)) - ch_mean * ch_mean
    ch_scale = bn_pair[0] * lax.rsqrt(ch_var + BN_EPS)
    return jnp.maximum((conv_out - ch_mean) * ch_scale + bn_pair[1], 0.0).astype(jnp.bfloat16)


def max_pool(hidden):
    return lax.reduce_window(hidden, jnp.array(-jnp.inf, hidden.dtype), lax.max, (1, 3, 3, 1), (1, 2, 2, 1), ((0, 0), (1, 1), (1, 1), (0, 0)))


def reference(pixels, w_stem, bn_stem, w_a, bn_a, w_down, bn_down, w_b, bn_b):
    hidden = max_pool(norm_relu(conv_full(pixels, w_stem, 2), bn_stem))

    def stage_step(carry, layer):
        kernel, bn_pair = layer
        return norm_relu(conv_full(carry, kernel, 1), bn_pair), None

    hidden, _ = lax.scan(stage_step, hidden, (w_a, bn_a))
    hidden = norm_relu(conv_full(hidden, w_down, 2), bn_down)
    hidden, _ = lax.scan(stage_step, hidden, (w_b, bn_b))
    return hidden
```

```python
import functools

import jax
import jax.numpy as jnp
from jax import lax
from jax.experimental import pallas as pl
from jax.experimental.pallas import tpu as pltpu
from jax.sharding import PartitionSpec as P

BN_EPS = 1e-5
F32 = jnp.float32
BF16 = jnp.bfloat16


def half_swap(x):
    return pltpu.roll(x, 64, x.ndim - 1)


def low_half(shape):
    return lax.broadcasted_iota(jnp.int32, shape, len(shape) - 1) < 64


def whole_kernel(group, counts, xk_ref, ws_ref, wa_ref, wd_ref, wb_ref, bns_ref, bna_ref, bnd_ref, bnb_ref, out_ref,
                 zs, za, ya, hb, yb, wat, wdt, acc, slots, ssend, srecv, hsend, hrecv):
    me = lax.axis_index("sp")
    nimg = za.shape[2]
    rows = za.shape[0]
    cols = za.shape[1]
    srows = zs.shape[0]
    orows = out_ref.shape[0]
    layers = wa_ref.shape[0]
    cnt_s, cnt_a, cnt_b = counts
    up, down = me - 1, me + 1

    barrier = pltpu.get_barrier_semaphore()
    for k in range(1, group):
        pl.semaphore_signal(barrier, inc=1, device_id={"sp": lax.rem(me + k, group)})

    def zero_rows(ref):
        @pl.loop(0, ref.shape[0])
        def _(r):
            ref[r] = jnp.zeros(ref.shape[1:], ref.dtype)

    zero_rows(ya)
    zero_rows(yb)
    hb[0] = jnp.zeros(hb.shape[1:], hb.dtype)

    @pl.loop(0, layers)
    def _(l):
        for r in range(4):
            for slot, t in enumerate((1, 2, 3, 0)):
                for dy in range(2):
                    ky = r - dy
                    parts = []
                    for dx in range(2):
                        kx = t - dx
                        if 0 <= ky < 3 and 0 <= kx < 3:
                            parts.append(wa_ref[l, ky, kx])
                        else:
                            parts.append(jnp.zeros((64, 64), BF16))
                    wat[l, pl.ds(r * 256 + slot * 64, 64), pl.ds(dy * 128, 128)] = jnp.concatenate(parts, axis=1)

    for r in range(3):
        for slot, kx in enumerate((1, 2, None, 0)):
            wdt[pl.ds(r * 256 + slot * 64, 64), :] = jnp.zeros((64, 128), BF16) if kx is None else wd_ref[r, kx]

    def clear_acc():
        acc[...] = jnp.zeros_like(acc)

    def add_acc(parts):
        s, q = acc[0], acc[1]
        for z in parts:
            z3 = z.reshape(z.shape[0] // 8, 8, z.shape[1])
            s = s + jnp.sum(z3, axis=0)
            q = q + jnp.sum(z3 * z3, axis=0)
        acc[0] = s
        acc[1] = q

    def stat_copy(par, k, source):
        block = slots.at[par, source]
        return pltpu.make_async_remote_copy(
            src_ref=block, dst_ref=block, send_sem=ssend.at[par, k], recv_sem=srecv.at[par, k],
            device_id={"sp": lax.rem(me + k, group)})

    def reduce_stats(par, bn, count, fold):
        s = jnp.sum(acc[0], axis=0, keepdims=True)
        q = jnp.sum(acc[1], axis=0, keepdims=True)
        slots[par, me] = jnp.concatenate([s, q, jnp.zeros((6, 128), F32)], axis=0)
        for k in range(1, group):
            stat_copy(par, k, me).start()
        for k in range(1, group):
            stat_copy(par, k, lax.rem(me + group - k, group)).wait_recv()
        for k in range(1, group):
            stat_copy(par, k, me).wait_send()
        total = slots[par, 0]
        for d in range(1, group):
            total = total + slots[par, d]
        if fold:
            total = total + half_swap(total)
        mean = total[0:1] / count
        var = total[1:2] / count - mean * mean
        scale = bn[0:1] * lax.rsqrt(var + BN_EPS)
        return mean, scale, bn[1:2]

    def apply(z, coef):
        mean, scale, beta = coef
        return jnp.maximum((z - mean) * scale + beta, 0.0)

    def send_up(buf, row, halo):
        return pltpu.make_async_remote_copy(
            src_ref=buf.at[row], dst_ref=buf.at[halo], send_sem=hsend.at[0], recv_sem=hrecv.at[0],
            device_id={"sp": up})

    def send_down(buf, row, halo):
        return pltpu.make_async_remote_copy(
            src_ref=buf.at[row], dst_ref=buf.at[halo], send_sem=hsend.at[1], recv_sem=hrecv.at[1],
            device_id={"sp": down})

    has_up, has_down = me > 0, me < group - 1

    def start_halos(buf, n):
        @pl.when(has_up)
        def _():
            send_up(buf, 1, n + 1).start()

        @pl.when(has_down)
        def _():
            send_down(buf, n, 0).start()

    def wait_halos(buf, n):
        @pl.when(has_up)
        def _():
            send_down(buf, n, 0).wait_recv()

        @pl.when(has_down)
        def _():
            send_up(buf, 1, n + 1).wait_recv()

    def drain_halos(buf, n):
        @pl.when(has_up)
        def _():
            send_up(buf, 1, n + 1).wait_send()

        @pl.when(has_down)
        def _():
            send_down(buf, n, 0).wait_send()

    clear_acc()
    pairs = srows + 3
    lanes = lax.broadcasted_iota(jnp.int32, (pairs, nimg, 128), 2)

    @pl.loop(0, xk_ref.shape[0])
    def _(kk):
        for jj in range(8):
            packed = None
            for r in range(2):
                for c in range(3):
                    off = r * 64 + c * 16
                    piece = xk_ref[kk, c, r]
                    shift = (off - 8 * jj) % 128
                    if shift:
                        piece = pltpu.roll(piece, shift, 2)
                    packed = piece if packed is None else jnp.where(lanes < off, packed, piece)
            lhs = jnp.concatenate([packed[p:p + srows].reshape(srows * nimg, 128) for p in range(4)], axis=1)
            z = jnp.dot(lhs, ws_ref[...], preferred_element_type=F32)
            j = kk * 8 + jj
            zl, zh = z[:, :128], z[:, 128:]
            zs[:, 0, pl.ds(j + 1, 1)] = zl.reshape(srows, 1, nimg, 128)
            zs[:, 1, pl.ds(j + 1, 1)] = zh.reshape(srows, 1, nimg, 128)
            add_acc([zl, zh])

    for h in range(srows):
        zs[h, 1, 0] = jnp.zeros((nimg, 128), F32)

    pl.semaphore_wait(barrier, group - 1)
    coef = reduce_stats(0, bns_ref[...], cnt_s, True)

    jp = 8

    def pool_row(h, jb):
        a = apply(zs[h, 0, pl.ds(jb * jp + 1, jp)], coef)
        b = apply(zs[h, 1, pl.ds(jb * jp, jp + 1)], coef)
        first = lax.broadcasted_iota(jnp.int32, b.shape, 0) + jb * jp
        b = jnp.where(first == 0, 0.0, b)
        rb = half_swap(b)
        lo = low_half(a.shape)
        m = jnp.maximum(a, jnp.where(lo, half_swap(a), rb[1:]))
        return jnp.maximum(m, jnp.where(lo, rb[:jp], b[1:]))

    def pool_pair(p):
        @pl.loop(0, cols // jp)
        def _(jb):
            top = pool_row(2 * p, jb)
            bot = pool_row(2 * p + 1, jb)
            hb[p + 1, pl.ds(jb * jp, jp)] = bot.astype(BF16)
            ya[p + 1, pl.ds(jb * jp + 1, jp)] = jnp.maximum(top, bot).astype(BF16)

    def pool_join(p):
        @pl.loop(0, cols // jp)
        def _(jb):
            old = ya[p + 1, pl.ds(jb * jp + 1, jp)]
            ya[p + 1, pl.ds(jb * jp + 1, jp)] = jnp.maximum(old, hb[p, pl.ds(jb * jp, jp)])

    pool_pair(rows - 1)

    def send_pool():
        return pltpu.make_async_remote_copy(
            src_ref=hb.at[rows], dst_ref=hb.at[0], send_sem=hsend.at[2], recv_sem=hrecv.at[2],
            device_id={"sp": down})

    @pl.when(has_down)
    def _():
        send_pool().start()

    @pl.loop(0, rows - 1)
    def _(p):
        pool_pair(p)

    @pl.loop(1, rows)
    def _(p):
        pool_join(p)

    @pl.when(has_up)
    def _():
        send_pool().wait_recv()

    pool_join(0)

    @pl.when(has_down)
    def _():
        send_pool().wait_send()

    start_halos(ya, rows)

    ja = 8

    def conv_a(l, i, jb):
        parts = []
        lo = low_half((ja, nimg, 128))
        for r in range(4):
            row = 2 * i + r
            mid = ya[row, pl.ds(jb * ja + 1, ja)]
            left = ya[row, pl.ds(jb * ja, ja)]
            right = ya[row, pl.ds(jb * ja + 2, ja)]
            parts.append(mid.reshape(ja * nimg, 128))
            parts.append(jnp.where(lo, right, left).reshape(ja * nimg, 128))
        z = jnp.dot(jnp.concatenate(parts, axis=1), wat[l], preferred_element_type=F32)
        for dy in range(2):
            za[2 * i + dy, pl.ds(jb * ja, ja)] = z[:, dy * 128:(dy + 1) * 128].reshape(ja, nimg, 128)
        add_acc([z[:, :128], z[:, 128:]])

    def norm_row(dst, row, coef):
        @pl.loop(0, cols // jp)
        def _(jb):
            dst[row + 1, pl.ds(jb * jp + 1, jp)] = apply(za[row, pl.ds(jb * jp, jp)], coef).astype(BF16)

    nblk = cols // ja

    @pl.loop(0, layers)
    def _(l):
        clear_acc()

        @pl.loop(0, (rows // 2 - 2) * nblk)
        def _(s):
            conv_a(l, 1 + lax.div(s, nblk), lax.rem(s, nblk))

        wait_halos(ya, rows)

        @pl.loop(0, 2 * nblk)
        def _(s):
            conv_a(l, lax.div(s, nblk) * (rows // 2 - 1), lax.rem(s, nblk))

        drain_halos(ya, rows)
        coef = reduce_stats(lax.rem(l + 1, 2), bna_ref[l], cnt_a, True)
        norm_row(ya, 0, coef)
        norm_row(ya, rows - 1, coef)
        start_halos(ya, rows)

        @pl.loop(1, rows - 1)
        def _(row):
            norm_row(ya, row, coef)

    clear_acc()
    jd = 16
    nblk_d = cols // jd

    def conv_d(i, jb):
        parts = []
        for r in range(3):
            row = 2 * i + r
            parts.append(ya[row, pl.ds(jb * jd + 1, jd)].reshape(jd * nimg, 128))
            parts.append(ya[row, pl.ds(jb * jd, jd)].reshape(jd * nimg, 128))
        z = jnp.dot(jnp.concatenate(parts, axis=1), wdt[...], preferred_element_type=F32)
        za[i, pl.ds(jb * jd, jd)] = z.reshape(jd, nimg, 128)
        add_acc([z])

    @pl.loop(0, (orows - 1) * nblk_d)
    def _(s):
        conv_d(1 + lax.div(s, nblk_d), lax.rem(s, nblk_d))

    wait_halos(ya, rows)

    @pl.loop(0, nblk_d)
    def _(jb):
        conv_d(0, jb)

    drain_halos(ya, rows)
    par = (layers + 1) % 2
    coef = reduce_stats(par, bnd_ref[...], cnt_b, False)

    def conv_b(l, i, jb):
        parts = []
        for r in range(3):
            for t in range(3):
                parts.append(yb[i + r, pl.ds(jb * jd + t, jd)].reshape(jd * nimg, 128))
        z = jnp.dot(jnp.concatenate(parts, axis=1), wb_ref[l], preferred_element_type=F32)
        za[i, pl.ds(jb * jd, jd)] = z.reshape(jd, nimg, 128)
        add_acc([z])

    for l in range(wb_ref.shape[0]):
        norm_row(yb, 0, coef)
        norm_row(yb, orows - 1, coef)
        start_halos(yb, orows)
        for row in range(1, orows - 1):
            norm_row(yb, row, coef)
        clear_acc()

        @pl.loop(0, (orows - 2) * nblk_d)
        def _(s):
            conv_b(l, 1 + lax.div(s, nblk_d), lax.rem(s, nblk_d))

        wait_halos(yb, orows)

        @pl.loop(0, 2 * nblk_d)
        def _(s):
            conv_b(l, lax.div(s, nblk_d) * (orows - 1), lax.rem(s, nblk_d))

        drain_halos(yb, orows)
        par = 1 - par
        coef = reduce_stats(par, bnb_ref[l], cnt_b, False)

    @pl.loop(0, orows)
    def _(row):
        @pl.loop(0, cols // jp)
        def _(jb):
            out_ref[row, pl.ds(jb * jp, jp)] = apply(za[row, pl.ds(jb * jp, jp)], coef).astype(BF16)


def stem_weights(w):
    w = jnp.pad(w, ((1, 0), (0, 0), (0, 1), (0, 0)))
    cols = [jnp.pad(w, ((0, 0), (2 * q + 1, 8 - 2 * q), (0, 0), (0, 0))) for q in range(4)]
    return jnp.concatenate(cols, axis=-1).transpose(0, 2, 1, 3).reshape(8 * 4 * 16, 256)


def solution(mesh):
    group = mesh.shape["sp"]

    def local_stack(pixels, w_stem, bn_stem, w_a, bn_a, w_down, bn_down, w_b, bn_b):
        n, h, w, chans = pixels.shape
        x = pixels.transpose(3, 1, 0, 2)
        above = lax.ppermute(x[:, -3:], "sp", [(i, i + 1) for i in range(group - 1)])
        below = lax.ppermute(x[:, :2], "sp", [(i + 1, i) for i in range(group - 1)])
        x = jnp.concatenate([jnp.zeros_like(x[:, :1]), above, x, below], axis=1)
        x = jnp.pad(x, ((0, 0), (0, 0), (0, 0), (4, 60)))
        hp = x.shape[1] // 2
        x = x.reshape(chans, hp, 2, n, (w + 64) // 64, 64).transpose(4, 0, 2, 1, 3, 5)
        xk = jnp.concatenate([x[:-1], x[1:]], axis=-1)
        rows, cols, orows = h // 4, w // 8, h // 8
        counts = (float(n * (h // 2) * group * (w // 2)), float(n * rows * group * (w // 4)), float(n * orows * group * (w // 8)))
        vm = pl.BlockSpec(memory_space=pltpu.VMEM)
        out = pl.pallas_call(
            functools.partial(whole_kernel, group, counts),
            out_shape=jax.ShapeDtypeStruct((orows, cols, n, 128), BF16),
            in_specs=[vm] * 9,
            out_specs=vm,
            scratch_shapes=[
                pltpu.VMEM((h // 2, 2, cols + 1, n, 128), F32),
                pltpu.VMEM((rows, cols, n, 128), F32),
                pltpu.VMEM((rows + 2, cols + 2, n, 128), BF16),
                pltpu.VMEM((rows + 1, cols, n, 128), BF16),
                pltpu.VMEM((orows + 2, cols + 2, n, 128), BF16),
                pltpu.VMEM((w_a.shape[0], 1024, 256), BF16),
                pltpu.VMEM((768, 128), BF16),
                pltpu.VMEM((2, 8, 128), F32),
                pltpu.VMEM((2, group, 8, 128), F32),
                pltpu.SemaphoreType.DMA((2, group)),
                pltpu.SemaphoreType.DMA((2, group)),
                pltpu.SemaphoreType.DMA((3,)),
                pltpu.SemaphoreType.DMA((3,)),
            ],
            compiler_params=pltpu.CompilerParams(collective_id=0, has_side_effects=True, vmem_limit_bytes=63 * 1024 * 1024),
        )(xk, stem_weights(w_stem), w_a, w_down, w_b.reshape(w_b.shape[0], 9 * 128, 128),
          jnp.tile(bn_stem, (1, 2)), jnp.tile(bn_a, (1, 1, 2)), bn_down, bn_b)
        return out.transpose(2, 0, 1, 3)

    return jax.shard_map(local_stack, mesh=mesh, in_specs=(P("dp", "sp"),) + (P(),) * 8, out_specs=P("dp", "sp"), check_vma=False)
```

```python
import functools

import jax
import jax.numpy as jnp
from jax import lax
from jax.experimental import pallas as pl
from jax.experimental.pallas import tpu as pltpu
from jax.sharding import PartitionSpec as P

BN_EPS = 1e-5
F32 = jnp.float32
BF16 = jnp.bfloat16


def half_swap(x):
    return pltpu.roll(x, 64, x.ndim - 1)


def low_half(shape):
    return lax.broadcasted_iota(jnp.int32, shape, len(shape) - 1) < 64


def whole_kernel(group, counts, x_ref, w7_ref, wa_ref, wd_ref, wb_ref, bns_ref, bna_ref, bnd_ref, bnb_ref, out_ref,
                 xt, xw, zs, za, zr, ya, hb, yb, wtmp, ws, wat, wdt, acc, slots, ssend, srecv, hsend, hrecv, psend, precv, zsend, zrecv):
    me = lax.axis_index("sp")
    nimg = za.shape[2]
    rows = za.shape[0]
    cols = za.shape[1]
    chunks, xpairs = xt.shape[0], xt.shape[1]
    own = xpairs - 4
    srows = own + 1
    orows = out_ref.shape[1]
    layers = wa_ref.shape[0]
    chans = x_ref.shape[1]
    cnt_s, cnt_a, cnt_b = counts
    up, down = me - 1, me + 1
    has_up, has_down = me > 0, me < group - 1
    even = lax.rem(me, 2) == 0
    odd = jnp.logical_not(even)

    for m in range(chunks):
        xt[m, 0:3] = jnp.zeros((3,) + xt.shape[2:], BF16)
        xt[m, xpairs - 1] = jnp.zeros(xt.shape[2:], BF16)

    barrier = pltpu.get_barrier_semaphore()
    for k in range(1, group):
        pl.semaphore_signal(barrier, inc=1, device_id={"sp": lax.rem(me + k, group)})

    @pl.loop(0, chans)
    def _(c):
        for h in range(own // 4):
            v = x_ref[:, c, pl.ds(8 * h, 8), :].astype(F32)
            v = jnp.transpose(v, (1, 0, 2)).astype(BF16)
            for m in range(chunks):
                for g in range(4):
                    for r in range(2):
                        xt[m, 3 + 4 * h + g, r, c] = v[2 * g + r, :, m * 128:(m + 1) * 128]

    def pix_down(m):
        return pltpu.make_async_remote_copy(
            src_ref=xt.at[m, pl.ds(own, 3)], dst_ref=xt.at[m, pl.ds(0, 3)], send_sem=psend.at[0, m], recv_sem=precv.at[0, m],
            device_id={"sp": down})

    def pix_up(m):
        return pltpu.make_async_remote_copy(
            src_ref=xt.at[m, pl.ds(3, 1)], dst_ref=xt.at[m, pl.ds(own + 3, 1)], send_sem=psend.at[1, m], recv_sem=precv.at[1, m],
            device_id={"sp": up})

    pl.semaphore_wait(barrier, group - 1)

    @pl.when(has_down)
    def _():
        for m in range(chunks):
            pix_down(m).start()

    @pl.when(has_up)
    def _():
        for m in range(chunks):
            pix_up(m).start()

    def zero_rows(ref):
        @pl.loop(0, ref.shape[0])
        def _(r):
            ref[r] = jnp.zeros(ref.shape[1:], ref.dtype)

    zero_rows(ya)
    zero_rows(yb)

    wtmp[...] = jnp.zeros_like(wtmp)
    ws[...] = jnp.zeros_like(ws)
    for ky in range(7):
        for c in range(chans):
            wtmp[pl.ds(8, 7), :] = w7_ref[ky, c].astype(F32)
            taps = [wtmp[pl.ds(7 - 2 * q, 16), :] for q in range(4)]
            ws[pl.ds((ky + 1) * 64 + c * 16, 16), :] = jnp.concatenate(taps, axis=1).astype(BF16)

    @pl.loop(0, layers)
    def _(l):
        for r in range(4):
            for slot, t in enumerate((1, 2, 3, 0)):
                for dy in range(2):
                    ky = r - dy
                    parts = []
                    for dx in range(2):
                        kx = t - dx
                        if 0 <= ky < 3 and 0 <= kx < 3:
                            parts.append(wa_ref[l, ky, kx])
                        else:
                            parts.append(jnp.zeros((64, 64), BF16))
                    wat[l, pl.ds(r * 256 + slot * 64, 64), pl.ds(dy * 128, 128)] = jnp.concatenate(parts, axis=1)

    for r in range(3):
        for slot, kx in enumerate((1, 2, None, 0)):
            wdt[pl.ds(r * 256 + slot * 64, 64), :] = jnp.zeros((64, 128), BF16) if kx is None else wd_ref[r, kx]

    def clear_acc():
        acc[...] = jnp.zeros_like(acc)

    def add_acc(parts):
        s, q = acc[0], acc[1]
        for z in parts:
            z3 = z.reshape(z.shape[0] // 8, 8, z.shape[1])
            s = s + jnp.sum(z3, axis=0)
            q = q + jnp.sum(z3 * z3, axis=0)
        acc[0] = s
        acc[1] = q

    def stat_copy(par, k, source):
        block = slots.at[par, source]
        return pltpu.make_async_remote_copy(
            src_ref=block, dst_ref=block, send_sem=ssend.at[par, k], recv_sem=srecv.at[par, k],
            device_id={"sp": lax.rem(me + k, group)})

    def reduce_stats(par, bn, count, fold, then=None):
        s = jnp.sum(acc[0], axis=0, keepdims=True)
        q = jnp.sum(acc[1], axis=0, keepdims=True)
        slots[par, me] = jnp.concatenate([s, q, jnp.zeros((6, 128), F32)], axis=0)
        for k in range(1, group):
            stat_copy(par, k, me).start()
        if then is not None:
            then()
        for k in range(1, group):
            stat_copy(par, k, lax.rem(me + group - k, group)).wait_recv()
        for k in range(1, group):
            stat_copy(par, k, me).wait_send()
        total = slots[par, 0]
        for d in range(1, group):
            total = total + slots[par, d]
        if fold:
            total = total + half_swap(total)
            bn = jnp.concatenate([bn, bn], axis=1)
        mean = total[0:1] / count
        var = total[1:2] / count - mean * mean
        scale = bn[0:1] * lax.rsqrt(var + BN_EPS)
        return mean, scale, bn[1:2]

    def apply(z, coef):
        mean, scale, beta = coef
        return jnp.maximum((z - mean) * scale + beta, 0.0)

    early = zr.shape[1]
    pieces = ((1, early), (1 + early, cols // 2 + 2 - early), (cols // 2 + 3, cols // 2 - 2), (1, cols))

    def halo(buf, n, side, which):
        src, dst, dev = (1, n + 1, up) if side == 0 else (n, 0, down)
        where = pl.ds(*pieces[which])
        return pltpu.make_async_remote_copy(
            src_ref=buf.at[src, where], dst_ref=buf.at[dst, where], send_sem=hsend.at[which], recv_sem=hrecv.at[which],
            device_id={"sp": dev})

    far_up, far_down = jnp.logical_and(even, has_up), jnp.logical_and(odd, has_down)
    near_up, near_down = jnp.logical_and(odd, has_up), jnp.logical_and(even, has_down)

    def far_op(op):
        @pl.when(far_up)
        def _():
            op(0, 1)

        @pl.when(far_down)
        def _():
            op(1, 0)

    def near_op(op):
        @pl.when(near_up)
        def _():
            op(0, 1)

        @pl.when(near_down)
        def _():
            op(1, 0)

    def start_far(buf, n, which):
        far_op(lambda out, back: [halo(buf, n, out, k).start() for k in which] and None)

    def wait_far(buf, n, which):
        far_op(lambda out, back: halo(buf, n, back, which).wait_recv())

    def sent_far(buf, n, which):
        far_op(lambda out, back: [halo(buf, n, out, k).wait_send() for k in which] and None)

    def start_near(buf, n):
        near_op(lambda out, back: halo(buf, n, out, 3).start())

    def wait_near(buf, n):
        near_op(lambda out, back: halo(buf, n, back, 3).wait_recv())

    def drain_halos(buf, n):
        sent_far(buf, n, (1, 2))
        near_op(lambda out, back: halo(buf, n, out, 3).wait_send())

    def early_copy(n, par, side):
        return pltpu.make_async_remote_copy(
            src_ref=za.at[0 if side == 0 else n - 1, pl.ds(0, early)], dst_ref=zr.at[par],
            send_sem=zsend.at[par], recv_sem=zrecv.at[par], device_id={"sp": up if side == 0 else down})

    def start_early(n, par):
        far_op(lambda out, back: early_copy(n, par, out).start())

    def finish_early(dst, n, par, coef):
        def take(out, back):
            early_copy(n, par, out).wait_recv()
            early_copy(n, par, out).wait_send()
            row = 0 if back == 1 else n + 1

            @pl.loop(0, early // 8)
            def _(jb):
                dst[row, pl.ds(jb * 8 + 1, 8)] = apply(zr[par, pl.ds(jb * 8, 8)], coef).astype(BF16)

        far_op(take)

    def far_near(n):
        return jnp.where(even, 0, n - 1), jnp.where(even, n - 1, 0)

    clear_acc()
    lanes = lax.broadcasted_iota(jnp.int32, (xpairs, nimg, 128), 2)

    def wait_pixels(m):
        @pl.when(has_up)
        def _():
            pix_down(m).wait_recv()

        @pl.when(has_down)
        def _():
            pix_up(m).wait_recv()

    wait_pixels(0)

    @pl.loop(0, 2 * chunks)
    def _(kk):
        first = lax.div(kk + 1, 2) - 1
        shift0 = 4 + 64 * lax.rem(kk, 2)

        @pl.when(jnp.logical_and(lax.rem(kk, 2) == 1, kk < 2 * chunks - 1))
        def _():
            wait_pixels(first + 1)

        low_ok = kk > 0
        high_ok = kk < 2 * chunks - 1
        left, right = jnp.maximum(first, 0), jnp.minimum(first + 1, chunks - 1)
        for r in range(2):
            for c in range(chans):
                off = r * 64 + c * 16
                rel = jnp.bitwise_and(lanes - off, 127)
                take_left = jnp.logical_and(rel < shift0, low_ok)
                take_right = jnp.logical_and(rel >= shift0, high_ok)
                shift = lax.rem(shift0 + off, 128)
                lv = pltpu.roll(xt[left, :, r, c], shift, 2)
                rv = pltpu.roll(xt[right, :, r, c], shift, 2)
                xw[r, c] = jnp.where(take_left, lv, jnp.where(take_right, rv, jnp.zeros_like(rv)))

        for jj in range(8):
            packed = None
            rel = jnp.bitwise_and(lanes - 8 * jj, 127)
            for r in range(2):
                for c in range(chans):
                    piece = xw[r, c]
                    packed = piece if packed is None else jnp.where(rel < r * 64 + c * 16, packed, piece)
            if jj:
                packed = pltpu.roll(packed, 128 - 8 * jj, 2)
            lhs = jnp.concatenate([packed[p:p + srows].reshape(srows * nimg, 128) for p in range(4)], axis=1)
            z = jnp.dot(lhs, ws[...], preferred_element_type=F32)
            j = kk * 8 + jj
            zl, zh = z[:, :128], z[:, 128:]
            zs[:, 0, pl.ds(j + 1, 1)] = zl.reshape(srows, 1, nimg, 128)
            zs[:, 1, pl.ds(j + 1, 1)] = zh.reshape(srows, 1, nimg, 128)
            add_acc([zl[nimg:], zh[nimg:]])

    for h in range(srows):
        zs[h, 1, 0] = jnp.zeros((nimg, 128), F32)

    coef = reduce_stats(0, bns_ref[...], cnt_s, True)

    jp = 8

    def pool_row(h, jb):
        a = apply(zs[h, 0, pl.ds(jb * jp + 1, jp)], coef).astype(BF16)
        b = apply(zs[h, 1, pl.ds(jb * jp, jp + 1)], coef)
        b = jnp.concatenate([jnp.where(jb > 0, b[:1], jnp.zeros_like(b[:1])), b[1:]], axis=0).astype(BF16)
        rb = half_swap(b)
        lo = low_half(a.shape)
        m = jnp.maximum(a, jnp.where(lo, half_swap(a), rb[1:]))
        return jnp.maximum(m, jnp.where(lo, rb[:jp], b[1:]))

    @pl.loop(0, cols // jp)
    def _(jb):
        top = pool_row(0, jb)
        hb[0, pl.ds(jb * jp, jp)] = jnp.where(has_up, top, jnp.zeros_like(top))

    def pool_pair(p):
        @pl.loop(0, cols // jp)
        def _(jb):
            top = pool_row(2 * p + 1, jb)
            bot = pool_row(2 * p + 2, jb)
            hb[p + 1, pl.ds(jb * jp, jp)] = bot
            ya[p + 1, pl.ds(jb * jp + 1, jp)] = jnp.maximum(top, bot)

    def pool_join(p):
        @pl.loop(0, cols // jp)
        def _(jb):
            old = ya[p + 1, pl.ds(jb * jp + 1, jp)]
            ya[p + 1, pl.ds(jb * jp + 1, jp)] = jnp.maximum(old, hb[p, pl.ds(jb * jp, jp)])

    far, near = far_near(rows)

    @pl.loop(0, 2)
    def _(t):
        pool_pair(jnp.where(even, t, rows - 2 + t))

    pool_join(far)
    start_far(ya, rows, (0, 1, 2))

    @pl.loop(2, rows)
    def _(t):
        pool_pair(jnp.where(even, t, t - 2))

    pool_join(near)
    start_near(ya, rows)

    @pl.loop(1, rows - 1)
    def _(p):
        pool_join(p)

    @pl.when(has_down)
    def _():
        for m in range(chunks):
            pix_down(m).wait_send()

    @pl.when(has_up)
    def _():
        for m in range(chunks):
            pix_up(m).wait_send()

    wait_far(ya, rows, 0)
    sent_far(ya, rows, (0,))

    ja = cols // 2

    def conv_a(l, i, jb):
        parts = []
        lo = low_half((ja, nimg, 128))
        for r in range(4):
            row = 2 * i + r
            mid = ya[row, pl.ds(jb * ja + 1, ja)]
            left = ya[row, pl.ds(jb * ja, ja)]
            right = ya[row, pl.ds(jb * ja + 2, ja)]
            parts.append(mid.reshape(ja * nimg, 128))
            parts.append(jnp.where(lo, right, left).reshape(ja * nimg, 128))
        z = jnp.dot(jnp.concatenate(parts, axis=1), wat[l], preferred_element_type=F32)
        for dy in range(2):
            za[2 * i + dy, pl.ds(jb * ja, ja)] = z[:, dy * 128:(dy + 1) * 128].reshape(ja, nimg, 128)
        add_acc([z[:, :128], z[:, 128:]])

    def norm_row(dst, row, coef):
        @pl.loop(0, cols // jp)
        def _(jb):
            dst[row + 1, pl.ds(jb * jp + 1, jp)] = apply(za[row, pl.ds(jb * jp, jp)], coef).astype(BF16)

    def norm_and_send(dst, n, coef, par):
        far, near = far_near(n)
        norm_row(dst, far, coef)
        start_far(dst, n, (1, 2))
        norm_row(dst, near, coef)
        start_near(dst, n)

        @pl.loop(1, n - 1)
        def _(row):
            norm_row(dst, row, coef)

        finish_early(dst, n, par, coef)

    def banded(conv, buf, n, blocks):
        far, near = far_near(blocks)

        @pl.loop(0, 2 * (blocks - 2))
        def _(s):
            conv(1 + lax.div(s, 2), lax.rem(s, 2))

        wait_near(buf, n)

        @pl.loop(0, 2)
        def _(s):
            conv(near, s)

        @pl.loop(0, 2)
        def _(s):
            @pl.when(s == 0)
            def _():
                wait_far(buf, n, 1)

            @pl.when(s == 1)
            def _():
                wait_far(buf, n, 2)

            conv(far, s)

        drain_halos(buf, n)

    @pl.loop(0, layers)
    def _(l):
        clear_acc()
        banded(functools.partial(conv_a, l), ya, rows, rows // 2)
        par = lax.rem(l + 1, 2)
        coef = reduce_stats(par, bna_ref[l], cnt_a, True, lambda: start_early(rows, par))
        norm_and_send(ya, rows, coef, par)

    clear_acc()
    jd = cols // 2

    def conv_d(i, jb):
        parts = []
        for r in range(3):
            row = 2 * i + r
            parts.append(ya[row, pl.ds(jb * jd + 1, jd)].reshape(jd * nimg, 128))
            parts.append(ya[row, pl.ds(jb * jd, jd)].reshape(jd * nimg, 128))
        z = jnp.dot(jnp.concatenate(parts, axis=1), wdt[...], preferred_element_type=F32)
        za[i, pl.ds(jb * jd, jd)] = z.reshape(jd, nimg, 128)
        add_acc([z])

    banded(conv_d, ya, rows, orows)
    par = (layers + 1) % 2
    coef = reduce_stats(par, bnd_ref[...], cnt_b, False, lambda: start_early(orows, par))

    def conv_b(l, i, jb):
        parts = []
        for r in range(3):
            for t in range(3):
                parts.append(yb[i + r, pl.ds(jb * jd + t, jd)].reshape(jd * nimg, 128))
        z = jnp.dot(jnp.concatenate(parts, axis=1), wb_ref[l], preferred_element_type=F32)
        za[i, pl.ds(jb * jd, jd)] = z.reshape(jd, nimg, 128)
        add_acc([z])

    for l in range(wb_ref.shape[0]):
        norm_and_send(yb, orows, coef, par)
        clear_acc()
        banded(functools.partial(conv_b, l), yb, orows, orows)
        par = 1 - par
        last = l == wb_ref.shape[0] - 1
        coef = reduce_stats(par, bnb_ref[l], cnt_b, False, None if last else lambda: start_early(orows, par))

    @pl.loop(0, orows)
    def _(row):
        for jb in range(cols // jp):
            y = apply(za[row, pl.ds(jb * jp, jp)], coef)
            out_ref[:, row, pl.ds(jb * jp, jp)] = jnp.transpose(y, (1, 0, 2)).astype(BF16)


def solution(mesh):
    group = mesh.shape["sp"]

    def local_stack(pixels, w_stem, bn_stem, w_a, bn_a, w_down, bn_down, w_b, bn_b):
        n, h, w, chans = pixels.shape
        rows, cols, orows = h // 4, w // 8, h // 8
        counts = (float(n * (h // 2) * group * (w // 2)), float(n * rows * group * (w // 4)), float(n * orows * group * (w // 8)))
        vm = pl.BlockSpec(memory_space=pltpu.VMEM)
        return pl.pallas_call(
            functools.partial(whole_kernel, group, counts),
            out_shape=jax.ShapeDtypeStruct((n, orows, cols, 128), BF16),
            in_specs=[vm] * 9,
            out_specs=vm,
            scratch_shapes=[
                pltpu.VMEM((w // 128, h // 2 + 4, 2, chans, n, 128), BF16),
                pltpu.VMEM((2, chans, h // 2 + 4, n, 128), BF16),
                pltpu.VMEM((h // 2 + 1, 2, cols + 1, n, 128), F32),
                pltpu.VMEM((rows, cols, n, 128), F32),
                pltpu.VMEM((2, cols // 2 - 8, n, 128), F32),
                pltpu.VMEM((rows + 2, cols + 2, n, 128), BF16),
                pltpu.VMEM((rows + 1, cols, n, 128), BF16),
                pltpu.VMEM((orows + 2, cols + 2, n, 128), BF16),
                pltpu.VMEM((32, 64), F32),
                pltpu.VMEM((512, 256), BF16),
                pltpu.VMEM((w_a.shape[0], 1024, 256), BF16),
                pltpu.VMEM((768, 128), BF16),
                pltpu.VMEM((2, 8, 128), F32),
                pltpu.VMEM((2, group, 8, 128), F32),
                pltpu.SemaphoreType.DMA((2, group)),
                pltpu.SemaphoreType.DMA((2, group)),
                pltpu.SemaphoreType.DMA((4,)),
                pltpu.SemaphoreType.DMA((4,)),
                pltpu.SemaphoreType.DMA((2, w // 128)),
                pltpu.SemaphoreType.DMA((2, w // 128)),
                pltpu.SemaphoreType.DMA((2,)),
                pltpu.SemaphoreType.DMA((2,)),
            ],
            compiler_params=pltpu.CompilerParams(collective_id=0, has_side_effects=True, vmem_limit_bytes=67_000_000),
        )(pixels.transpose(0, 3, 1, 2), w_stem.transpose(0, 2, 1, 3), w_a, w_down, w_b.reshape(w_b.shape[0], 9 * 128, 128),
          bn_stem, bn_a, bn_down, bn_b)

    return jax.shard_map(local_stack, mesh=mesh, in_specs=(P("dp", "sp"),) + (P(),) * 8, out_specs=P("dp", "sp"), check_vma=False)
```

```python
import functools

import jax
import jax.numpy as jnp
from jax import lax
from jax.experimental import pallas as pl
from jax.experimental.pallas import tpu as pltpu
from jax.sharding import PartitionSpec as P

BN_EPS = 1e-5
F32 = jnp.float32
BF16 = jnp.bfloat16


def half_swap(x):
    return pltpu.roll(x, 64, x.ndim - 1)


def low_half(shape):
    return lax.broadcasted_iota(jnp.int32, shape, len(shape) - 1) < 64


def whole_kernel(group, counts, x_ref, w7_ref, wa_ref, wd_ref, wb_ref, bns_ref, bna_ref, bnd_ref, bnb_ref, out_ref,
                 xt, xw, zs, za, zr, ya, hb, yb, wtmp, ws, wat, wdt, acc, slots, ssend, srecv, hsend, hrecv, psend, precv, zsend, zrecv):
    me = lax.axis_index("sp")
    nimg = za.shape[2]
    rows = za.shape[0]
    cols = za.shape[1]
    chunks, xpairs = xt.shape[0], xt.shape[1]
    own = xpairs - 4
    srows = own + 1
    orows = out_ref.shape[1]
    layers = wa_ref.shape[0]
    chans = x_ref.shape[1]
    cnt_s, cnt_a, cnt_b = counts
    up, down = me - 1, me + 1
    has_up, has_down = me > 0, me < group - 1
    even = lax.rem(me, 2) == 0
    odd = jnp.logical_not(even)

    for m in range(chunks):
        xt[m, 0:3] = jnp.zeros((3,) + xt.shape[2:], BF16)
        xt[m, xpairs - 1] = jnp.zeros(xt.shape[2:], BF16)

    barrier = pltpu.get_barrier_semaphore()
    for k in range(1, group):
        pl.semaphore_signal(barrier, inc=1, device_id={"sp": lax.rem(me + k, group)})

    @pl.loop(0, chans)
    def _(c):
        for h in range(own // 4):
            v = x_ref[:, c, pl.ds(8 * h, 8), :].astype(F32)
            v = jnp.transpose(v, (1, 0, 2)).astype(BF16)
            for m in range(chunks):
                for g in range(4):
                    for r in range(2):
                        xt[m, 3 + 4 * h + g, r, c] = v[2 * g + r, :, m * 128:(m + 1) * 128]

    def pix_down(m):
        return pltpu.make_async_remote_copy(
            src_ref=xt.at[m, pl.ds(own, 3)], dst_ref=xt.at[m, pl.ds(0, 3)], send_sem=psend.at[0, m], recv_sem=precv.at[0, m],
            device_id={"sp": down})

    def pix_up(m):
        return pltpu.make_async_remote_copy(
            src_ref=xt.at[m, pl.ds(3, 1)], dst_ref=xt.at[m, pl.ds(own + 3, 1)], send_sem=psend.at[1, m], recv_sem=precv.at[1, m],
            device_id={"sp": up})

    pl.semaphore_wait(barrier, group - 1)

    @pl.when(has_down)
    def _():
        for m in range(chunks):
            pix_down(m).start()

    @pl.when(has_up)
    def _():
        for m in range(chunks):
            pix_up(m).start()

    def zero_rows(ref):
        @pl.loop(0, ref.shape[0])
        def _(r):
            ref[r] = jnp.zeros(ref.shape[1:], ref.dtype)

    zero_rows(ya)
    zero_rows(yb)

    wtmp[...] = jnp.zeros_like(wtmp)
    ws[...] = jnp.zeros_like(ws)
    for ky in range(7):
        for c in range(chans):
            wtmp[pl.ds(8, 7), :] = w7_ref[ky, c].astype(F32)
            taps = [wtmp[pl.ds(7 - 2 * q, 16), :] for q in range(4)]
            ws[pl.ds((ky + 1) * 64 + c * 16, 16), :] = jnp.concatenate(taps, axis=1).astype(BF16)

    @pl.loop(0, layers)
    def _(l):
        for r in range(4):
            for slot, t in enumerate((1, 2, 3, 0)):
                for dy in range(2):
                    ky = r - dy
                    parts = []
                    for dx in range(2):
                        kx = t - dx
                        if 0 <= ky < 3 and 0 <= kx < 3:
                            parts.append(wa_ref[l, ky, kx])
                        else:
                            parts.append(jnp.zeros((64, 64), BF16))
                    wat[l, pl.ds(r * 256 + slot * 64, 64), pl.ds(dy * 128, 128)] = jnp.concatenate(parts, axis=1)

    for r in range(3):
        for slot, kx in enumerate((1, 2, None, 0)):
            wdt[pl.ds(r * 256 + slot * 64, 64), :] = jnp.zeros((64, 128), BF16) if kx is None else wd_ref[r, kx]

    def clear_acc():
        acc[...] = jnp.zeros_like(acc)

    def add_acc(parts):
        s, q = acc[0], acc[1]
        for z in parts:
            z3 = z.reshape(z.shape[0] // 8, 8, z.shape[1])
            s = s + jnp.sum(z3, axis=0)
            q = q + jnp.sum(z3 * z3, axis=0)
        acc[0] = s
        acc[1] = q

    def stat_copy(par, k, source):
        block = slots.at[par, source]
        return pltpu.make_async_remote_copy(
            src_ref=block, dst_ref=block, send_sem=ssend.at[par, k], recv_sem=srecv.at[par, k],
            device_id={"sp": lax.rem(me + k, group)})

    def reduce_stats(par, bn, count, fold, then=None):
        s = jnp.sum(acc[0], axis=0, keepdims=True)
        q = jnp.sum(acc[1], axis=0, keepdims=True)
        slots[par, me] = jnp.concatenate([s, q], axis=0)
        for k in sorted(range(1, group), key=lambda d: abs(2 * d - group)):
            stat_copy(par, k, me).start()
        if then is not None:
            then()
        for k in range(1, group):
            stat_copy(par, k, lax.rem(me + group - k, group)).wait_recv()
        for k in range(1, group):
            stat_copy(par, k, me).wait_send()
        total = slots[par, 0]
        for d in range(1, group):
            total = total + slots[par, d]
        if fold:
            total = total + half_swap(total)
            bn = jnp.concatenate([bn, bn], axis=1)
        mean = total[0:1] / count
        var = total[1:2] / count - mean * mean
        scale = bn[0:1] * lax.rsqrt(var + BN_EPS)
        return mean, scale, bn[1:2]

    def apply(z, coef):
        mean, scale, beta = coef
        return jnp.maximum((z - mean) * scale + beta, 0.0)

    early = zr.shape[1]
    pieces = ((1, early), (1 + early, cols // 2 + 2 - early), (cols // 2 + 3, cols // 2 - 2), (1, cols))

    def halo(buf, n, side, which):
        src, dst, dev = (1, n + 1, up) if side == 0 else (n, 0, down)
        where = pl.ds(*pieces[which])
        return pltpu.make_async_remote_copy(
            src_ref=buf.at[src, where], dst_ref=buf.at[dst, where], send_sem=hsend.at[which], recv_sem=hrecv.at[which],
            device_id={"sp": dev})

    far_up, far_down = jnp.logical_and(even, has_up), jnp.logical_and(odd, has_down)
    near_up, near_down = jnp.logical_and(odd, has_up), jnp.logical_and(even, has_down)

    def far_op(op):
        @pl.when(far_up)
        def _():
            op(0, 1)

        @pl.when(far_down)
        def _():
            op(1, 0)

    def near_op(op):
        @pl.when(near_up)
        def _():
            op(0, 1)

        @pl.when(near_down)
        def _():
            op(1, 0)

    def start_far(buf, n, which):
        far_op(lambda out, back: [halo(buf, n, out, k).start() for k in which] and None)

    def wait_far(buf, n, which):
        far_op(lambda out, back: halo(buf, n, back, which).wait_recv())

    def sent_far(buf, n, which):
        far_op(lambda out, back: [halo(buf, n, out, k).wait_send() for k in which] and None)

    def start_near(buf, n):
        near_op(lambda out, back: halo(buf, n, out, 3).start())

    def wait_near(buf, n):
        near_op(lambda out, back: halo(buf, n, back, 3).wait_recv())

    def drain_halos(buf, n):
        sent_far(buf, n, (1, 2))
        near_op(lambda out, back: halo(buf, n, out, 3).wait_send())

    def early_copy(n, par, side):
        return pltpu.make_async_remote_copy(
            src_ref=za.at[0 if side == 0 else n - 1, pl.ds(0, early)], dst_ref=zr.at[par],
            send_sem=zsend.at[par], recv_sem=zrecv.at[par], device_id={"sp": up if side == 0 else down})

    def start_early(n, par):
        far_op(lambda out, back: early_copy(n, par, out).start())

    def finish_early(dst, n, par, coef):
        def take(out, back):
            early_copy(n, par, out).wait_recv()
            early_copy(n, par, out).wait_send()
            row = 0 if back == 1 else n + 1

            @pl.loop(0, early // 8)
            def _(jb):
                dst[row, pl.ds(jb * 8 + 1, 8)] = apply(zr[par, pl.ds(jb * 8, 8)], coef).astype(BF16)

        far_op(take)

    def far_near(n):
        return jnp.where(even, 0, n - 1), jnp.where(even, n - 1, 0)

    clear_acc()
    lanes = lax.broadcasted_iota(jnp.int32, (xpairs, nimg, 128), 2)

    def wait_pixels(m):
        @pl.when(has_up)
        def _():
            pix_down(m).wait_recv()

        @pl.when(has_down)
        def _():
            pix_up(m).wait_recv()

    wait_pixels(0)

    @pl.loop(0, 2 * chunks)
    def _(kk):
        first = lax.div(kk + 1, 2) - 1
        shift0 = 4 + 64 * lax.rem(kk, 2)

        @pl.when(jnp.logical_and(lax.rem(kk, 2) == 1, kk < 2 * chunks - 1))
        def _():
            wait_pixels(first + 1)

        low_ok = kk > 0
        high_ok = kk < 2 * chunks - 1
        left, right = jnp.maximum(first, 0), jnp.minimum(first + 1, chunks - 1)
        for r in range(2):
            for c in range(chans):
                off = r * 64 + c * 16
                rel = jnp.bitwise_and(lanes - off, 127)
                take_left = jnp.logical_and(rel < shift0, low_ok)
                take_right = jnp.logical_and(rel >= shift0, high_ok)
                shift = lax.rem(shift0 + off, 128)
                lv = pltpu.roll(xt[left, :, r, c], shift, 2)
                rv = pltpu.roll(xt[right, :, r, c], shift, 2)
                xw[r, c] = jnp.where(take_left, lv, jnp.where(take_right, rv, jnp.zeros_like(rv)))

        for jj in range(8):
            packed = None
            rel = jnp.bitwise_and(lanes - 8 * jj, 127)
            for r in range(2):
                for c in range(chans):
                    piece = xw[r, c]
                    packed = piece if packed is None else jnp.where(rel < r * 64 + c * 16, packed, piece)
            if jj:
                packed = pltpu.roll(packed, 128 - 8 * jj, 2)
            lhs = jnp.concatenate([packed[p:p + srows].reshape(srows * nimg, 128) for p in range(4)], axis=1)
            z = jnp.dot(lhs, ws[...], preferred_element_type=F32)
            j = kk * 8 + jj
            zl, zh = z[:, :128], z[:, 128:]
            zs[:, 0, pl.ds(j + 1, 1)] = zl.reshape(srows, 1, nimg, 128)
            zs[:, 1, pl.ds(j + 1, 1)] = zh.reshape(srows, 1, nimg, 128)
            add_acc([zl[nimg:], zh[nimg:]])

    for h in range(srows):
        zs[h, 1, 0] = jnp.zeros((nimg, 128), F32)

    coef = reduce_stats(0, bns_ref[...], cnt_s, True)

    jp = 8

    def pool_row(h, jb):
        a = apply(zs[h, 0, pl.ds(jb * jp + 1, jp)], coef).astype(BF16)
        b = apply(zs[h, 1, pl.ds(jb * jp, jp + 1)], coef)
        b = jnp.concatenate([jnp.where(jb > 0, b[:1], jnp.zeros_like(b[:1])), b[1:]], axis=0).astype(BF16)
        rb = half_swap(b)
        lo = low_half(a.shape)
        m = jnp.maximum(a, jnp.where(lo, half_swap(a), rb[1:]))
        return jnp.maximum(m, jnp.where(lo, rb[:jp], b[1:]))

    @pl.loop(0, cols // jp)
    def _(jb):
        top = pool_row(0, jb)
        hb[0, pl.ds(jb * jp, jp)] = jnp.where(has_up, top, jnp.zeros_like(top))

    def pool_pair(p):
        @pl.loop(0, cols // jp)
        def _(jb):
            top = pool_row(2 * p + 1, jb)
            bot = pool_row(2 * p + 2, jb)
            hb[p + 1, pl.ds(jb * jp, jp)] = bot
            ya[p + 1, pl.ds(jb * jp + 1, jp)] = jnp.maximum(top, bot)

    def pool_join(p):
        @pl.loop(0, cols // jp)
        def _(jb):
            old = ya[p + 1, pl.ds(jb * jp + 1, jp)]
            ya[p + 1, pl.ds(jb * jp + 1, jp)] = jnp.maximum(old, hb[p, pl.ds(jb * jp, jp)])

    far, near = far_near(rows)

    @pl.loop(0, 2)
    def _(t):
        pool_pair(jnp.where(even, t, rows - 2 + t))

    pool_join(far)
    start_far(ya, rows, (0, 1, 2))

    @pl.loop(2, rows)
    def _(t):
        pool_pair(jnp.where(even, t, t - 2))

    pool_join(near)
    start_near(ya, rows)

    @pl.loop(1, rows - 1)
    def _(p):
        pool_join(p)

    @pl.when(has_down)
    def _():
        for m in range(chunks):
            pix_down(m).wait_send()

    @pl.when(has_up)
    def _():
        for m in range(chunks):
            pix_up(m).wait_send()

    wait_far(ya, rows, 0)
    sent_far(ya, rows, (0,))

    ja = cols // 2

    def conv_a(l, i, jb):
        parts = []
        lo = low_half((ja, nimg, 128))
        for r in range(4):
            row = 2 * i + r
            mid = ya[row, pl.ds(jb * ja + 1, ja)]
            left = ya[row, pl.ds(jb * ja, ja)]
            right = ya[row, pl.ds(jb * ja + 2, ja)]
            parts.append(mid.reshape(ja * nimg, 128))
            parts.append(jnp.where(lo, right, left).reshape(ja * nimg, 128))
        z = jnp.dot(jnp.concatenate(parts, axis=1), wat[l], preferred_element_type=F32)
        for dy in range(2):
            za[2 * i + dy, pl.ds(jb * ja, ja)] = z[:, dy * 128:(dy + 1) * 128].reshape(ja, nimg, 128)
        add_acc([z[:, :128], z[:, 128:]])

    def norm_row(dst, row, coef):
        @pl.loop(0, cols // jp)
        def _(jb):
            dst[row + 1, pl.ds(jb * jp + 1, jp)] = apply(za[row, pl.ds(jb * jp, jp)], coef).astype(BF16)

    def norm_and_send(dst, n, coef):
        far, near = far_near(n)
        norm_row(dst, far, coef)
        start_far(dst, n, (1, 2))
        norm_row(dst, near, coef)
        start_near(dst, n)

        @pl.loop(1, n - 1)
        def _(row):
            norm_row(dst, row, coef)

    def banded(conv, buf, n, blocks, arrived=None):
        far, near = far_near(blocks)

        @pl.loop(0, 2 * (blocks - 2))
        def _(s):
            conv(1 + lax.div(s, 2), lax.rem(s, 2))

        wait_near(buf, n)

        @pl.loop(0, 2)
        def _(s):
            conv(near, s)

        if arrived is not None:
            arrived()

        @pl.loop(0, 2)
        def _(s):
            @pl.when(s == 0)
            def _():
                wait_far(buf, n, 1)

            @pl.when(s == 1)
            def _():
                wait_far(buf, n, 2)

            conv(far, s)

        drain_halos(buf, n)

    def finish_a(l):
        par = lax.rem(l + 1, 2)
        coef = reduce_stats(par, bna_ref[l], cnt_a, True, lambda: start_early(rows, par))
        norm_and_send(ya, rows, coef)
        clear_acc()
        return lambda: finish_early(ya, rows, par, coef)

    clear_acc()
    banded(functools.partial(conv_a, 0), ya, rows, rows // 2)

    @pl.loop(1, layers)
    def _(l):
        arrived = finish_a(l - 1)
        banded(functools.partial(conv_a, l), ya, rows, rows // 2, arrived)

    arrived = finish_a(layers - 1)

    jd = cols // 2

    def conv_d(i, jb):
        parts = []
        for r in range(3):
            row = 2 * i + r
            parts.append(ya[row, pl.ds(jb * jd + 1, jd)].reshape(jd * nimg, 128))
            parts.append(ya[row, pl.ds(jb * jd, jd)].reshape(jd * nimg, 128))
        z = jnp.dot(jnp.concatenate(parts, axis=1), wdt[...], preferred_element_type=F32)
        za[i, pl.ds(jb * jd, jd)] = z.reshape(jd, nimg, 128)
        add_acc([z])

    banded(conv_d, ya, rows, orows, arrived)
    par = (layers + 1) % 2
    coef = reduce_stats(par, bnd_ref[...], cnt_b, False, lambda: start_early(orows, par))

    def conv_b(l, i, jb):
        parts = []
        for r in range(3):
            for t in range(3):
                parts.append(yb[i + r, pl.ds(jb * jd + t, jd)].reshape(jd * nimg, 128))
        z = jnp.dot(jnp.concatenate(parts, axis=1), wb_ref[l], preferred_element_type=F32)
        za[i, pl.ds(jb * jd, jd)] = z.reshape(jd, nimg, 128)
        add_acc([z])

    for l in range(wb_ref.shape[0]):
        norm_and_send(yb, orows, coef)
        clear_acc()
        banded(functools.partial(conv_b, l), yb, orows, orows, functools.partial(finish_early, yb, orows, par, coef))
        par = 1 - par
        last = l == wb_ref.shape[0] - 1
        coef = reduce_stats(par, bnb_ref[l], cnt_b, False, None if last else lambda: start_early(orows, par))

    @pl.loop(0, orows)
    def _(row):
        for jb in range(cols // jp):
            y = apply(za[row, pl.ds(jb * jp, jp)], coef)
            out_ref[:, row, pl.ds(jb * jp, jp)] = jnp.transpose(y, (1, 0, 2)).astype(BF16)


def solution(mesh):
    group = mesh.shape["sp"]

    def local_stack(pixels, w_stem, bn_stem, w_a, bn_a, w_down, bn_down, w_b, bn_b):
        n, h, w, chans = pixels.shape
        rows, cols, orows = h // 4, w // 8, h // 8
        counts = (float(n * (h // 2) * group * (w // 2)), float(n * rows * group * (w // 4)), float(n * orows * group * (w // 8)))
        vm = pl.BlockSpec(memory_space=pltpu.VMEM)
        return pl.pallas_call(
            functools.partial(whole_kernel, group, counts),
            out_shape=jax.ShapeDtypeStruct((n, orows, cols, 128), BF16),
            in_specs=[vm] * 9,
            out_specs=vm,
            scratch_shapes=[
                pltpu.VMEM((w // 128, h // 2 + 4, 2, chans, n, 128), BF16),
                pltpu.VMEM((2, chans, h // 2 + 4, n, 128), BF16),
                pltpu.VMEM((h // 2 + 1, 2, cols + 1, n, 128), F32),
                pltpu.VMEM((rows, cols, n, 128), F32),
                pltpu.VMEM((2, cols // 2 - 8, n, 128), F32),
                pltpu.VMEM((rows + 2, cols + 2, n, 128), BF16),
                pltpu.VMEM((rows + 1, cols, n, 128), BF16),
                pltpu.VMEM((orows + 2, cols + 2, n, 128), BF16),
                pltpu.VMEM((32, 64), F32),
                pltpu.VMEM((512, 256), BF16),
                pltpu.VMEM((w_a.shape[0], 1024, 256), BF16),
                pltpu.VMEM((768, 128), BF16),
                pltpu.VMEM((2, 8, 128), F32),
                pltpu.VMEM((2, group, 2, 128), F32),
                pltpu.SemaphoreType.DMA((2, group)),
                pltpu.SemaphoreType.DMA((2, group)),
                pltpu.SemaphoreType.DMA((4,)),
                pltpu.SemaphoreType.DMA((4,)),
                pltpu.SemaphoreType.DMA((2, w // 128)),
                pltpu.SemaphoreType.DMA((2, w // 128)),
                pltpu.SemaphoreType.DMA((2,)),
                pltpu.SemaphoreType.DMA((2,)),
            ],
            compiler_params=pltpu.CompilerParams(collective_id=0, has_side_effects=True, vmem_limit_bytes=67_000_000),
        )(pixels.transpose(0, 3, 1, 2), w_stem.transpose(0, 2, 1, 3), w_a, w_down, w_b.reshape(w_b.shape[0], 9 * 128, 128),
          bn_stem, bn_a, bn_down, bn_b)

    return jax.shard_map(local_stack, mesh=mesh, in_specs=(P("dp", "sp"),) + (P(),) * 8, out_specs=P("dp", "sp"), check_vma=False)
```
